256 devices in a mesh: row: 64 (over x_hi, y, z), col: 4 (over x_lo, core).
Axes of the slice: x: 4 (x_hi: 2, x_lo: 2; x = x_hi * 2 + x_lo), y: 4, z: 8, core: 2. Of those that a mesh axis runs over, the one named last changes fastest.
Arguments:
- tables: bfloat16 [256, 8192, 256], P(('row', 'col')), may hold values from -1.78125 to 1.78125, as said below
- bags: int32 [256, 8, 1024], P('row'), may hold values from 0 to 8191
- old_map: int32 [256], replicated, may hold values from 0 to 255, each once
- new_map: int32 [256], replicated, may hold values from 0 to 255, each once
Outputs:
- features: bfloat16 [1024, 256, 256], P('row', None, 'col')
The draws below stay inside these ranges and needn't reach their ends.
Inputs may be any that keep to these rules, and one draw needn't show every extreme that they name: `tables`: every entry is a whole multiple of 1/64. `old_map`: a permutation of the table ids. `new_map`: a permutation of the output positions.
All inputs are finite; a program needn't handle non-finite values. Where the reference program divides by a largest or mean magnitude, that divisor is 1e-20 or more.
Results may differ from the reference program's by a relative error of at most 0.01.
Values may be sent and summed in bfloat16 or wider, within the bound.
A program may use at most 64 MiB of HBM per device.

```python
import jax
import jax.numpy as jnp
from jax import lax

ROWS = 8192
DIM = 256
POOL = 8
BATCH = 1024
TABLES = 256
N_COL = 4


def draw_tables(key, part):
    shape = (TABLES, ROWS, DIM)
    keys = jax.random.split(jax.random.fold_in(key, 11), 1)
    value = jax.random.randint(keys[0], shape, -57, 58).astype(jnp.float32)
    return (value / 64.0).astype(jnp.bfloat16)


def place_ends(drawn, key, low, high):
    index_at = [jax.random.randint(jax.random.fold_in(key, axis), (), 0, length) for axis, length in enumerate(drawn.shape)]
    main_axis = drawn.shape.index(max(drawn.shape))
    next_to = index_at[:main_axis] + [(index_at[main_axis] + 1) % drawn.shape[main_axis]] + index_at[main_axis + 1:]
    return drawn.at[tuple(index_at)].set(low).at[tuple(next_to)].set(high)


def setup_inputs(seed: int = 0) -> dict:
    splits = jax.random.split(jax.random.key(seed), 5)
    return {
        "tables": draw_tables(jax.random.fold_in(splits[4], 71), 0),
        "bags": place_ends(jax.random.randint(splits[1], (TABLES, POOL, BATCH), 0, ROWS), jax.random.fold_in(splits[1], 1), 0, ROWS - 1).astype(jnp.int32),
        "old_map": jax.random.permutation(splits[2], TABLES).astype(jnp.int32),
        "new_map": jax.random.permutation(splits[3], TABLES).astype(jnp.int32),
    }


def restore_one(operands):
    embedding, bag_rows = operands
    pooled = jnp.sum(jnp.take(embedding, bag_rows, axis=0).astype(jnp.float32), axis=0)
    pieces = pooled.reshape(BATCH, N_COL, DIM // N_COL)
    scale = jnp.max(jnp.abs(pieces), axis=2, keepdims=True) + 0.0078125
    levels = jnp.floor((pieces * 127.0) / scale + 0.5).astype(jnp.bfloat16)
    restored = ((levels.astype(jnp.float32) * scale) / 127.0).astype(jnp.bfloat16)
    return restored.reshape(BATCH, DIM)


def reference(tables, bags, old_map, new_map):
    restored = lax.map(restore_one, (tables, bags))
    position = new_map[old_map]
    inverse = jnp.zeros((TABLES,), jnp.int32).at[position].set(jnp.arange(TABLES, dtype=jnp.int32))
    ordered = jnp.take(restored, inverse, axis=0)
    return jnp.swapaxes(ordered, 0, 1)
```

```python
import functools

import jax
import jax.numpy as jnp
from jax import lax
from jax.experimental import pallas as pl
from jax.experimental.pallas import tpu as pltpu
from jax.sharding import PartitionSpec as P

MESH = pl.DeviceIdType.MESH
HIGH = 4096.0


def signed_step(index):
    half = lax.div(index + 1, 2)
    return jnp.where(lax.rem(index, 2) == 1, half, -half)


def pool_and_send(dims, bags_ref, table_ref, recv_ref, bags, raw, packed, pooled, send, bag_sem, table_sem, send_sem, recv_sem):
    rows, cols, per_row, pool, chunks = dims
    row, col = lax.axis_index("row"), lax.axis_index("col")
    me = row * cols + col
    total = rows * cols
    chunk = raw.shape[0] // chunks

    def table_copy(c):
        part = pl.ds(c * chunk, chunk)
        return pltpu.make_async_copy(table_ref.at[0, part, :], raw.at[part, :], table_sem.at[c])

    bag_copy = pltpu.make_async_copy(bags_ref.at[col], bags, bag_sem)
    bag_copy.start()
    for c in range(chunks):
        table_copy(c).start()

    barrier = pltpu.get_barrier_semaphore()

    def greet(i, _):
        other = lax.rem(me + i, total)
        pl.semaphore_signal(
            barrier, inc=1, device_id=(lax.div(other, cols), lax.rem(other, cols)), device_id_type=MESH
        )
        return 0

    lax.fori_loop(1, total, greet, 0)

    for c in range(chunks):
        table_copy(c).wait()

        def pack(i, _):
            at = pl.ds(pl.multiple_of(c * chunk + i * 64, 64), 64)
            pair = raw[at, :].astype(jnp.float32)
            packed[at, :] = pair[:, :128] + pair[:, 128:] * HIGH
            return 0

        lax.fori_loop(0, chunk // 64, pack, 0)
    bag_copy.wait()

    def destination(i):
        step = lax.rem(row + 1 + i, rows)
        return step

    def gather(i):
        base = destination(i) * per_row
        for j in range(per_row):
            total_row = packed[pl.ds(bags[0, base + j], 1), :]
            for l in range(1, pool):
                total_row = total_row + packed[pl.ds(bags[l, base + j], 1), :]
            pooled[pl.ds(j, 1), :] = total_row
        return pooled[0:8, :], pooled[8:16, :]

    def quantize(i, sums):
        first = lax.broadcasted_iota(jnp.int32, (8, 128), 1) < 64
        halves = []
        for s in sums:
            high = jnp.floor(s * (64.0 / HIGH) + 0.5)
            halves.append((s - high * (HIGH / 64.0), high * (1.0 / 64.0)))
        target = destination(i) * cols
        for k in range(4):
            top, bottom = halves[0][k // 2], halves[1][k // 2]
            if k % 2 == 0:
                block = jnp.where(first, top, pltpu.roll(bottom, 64, 1))
            else:
                block = jnp.where(first, pltpu.roll(top, 64, 1), bottom)
            size = jnp.abs(block)
            left = jnp.max(jnp.where(first, size, 0.0), axis=1, keepdims=True)
            right = jnp.max(jnp.where(first, 0.0, size), axis=1, keepdims=True)
            scale = jnp.where(first, left, right) + 0.0078125
            levels = jnp.floor(block * (127.0 / scale) + 0.5)
            send[target + k] = (levels * scale / 127.0).astype(jnp.bfloat16)

    def copy_to(r, k):
        return pltpu.make_async_remote_copy(
            src_ref=send.at[r * cols + k],
            dst_ref=recv_ref.at[me],
            send_sem=send_sem,
            recv_sem=recv_sem,
            device_id=(r, k),
            device_id_type=MESH,
        )

    def send_all(i):
        r = destination(i)
        for k in range(4):
            copy_to(r, k).start()

    sums = gather(0)
    quantize(0, sums)
    sums = gather(1)
    pl.semaphore_wait(barrier, total - 1)

    def body(i, sums):
        send_all(i - 2)
        quantize(i - 1, sums)
        return gather(i)

    sums = lax.fori_loop(2, rows, body, sums)
    send_all(rows - 2)
    quantize(rows - 1, sums)
    recv_ref[me] = send[me]
    for k in range(4):

        @pl.when(col != k)
        def _():
            copy_to(row, k).start()

    others = pl.ds(0, total - 1)
    done = pltpu.make_async_remote_copy(
        src_ref=send.at[others],
        dst_ref=recv_ref.at[others],
        send_sem=send_sem,
        recv_sem=recv_sem,
        device_id=(row, lax.rem(col + 1, cols)),
        device_id_type=MESH,
    )
    done.wait()


def place(old_ref, new_ref, recv_ref, out_ref, wide):
    total = recv_ref.shape[0]
    at = lax.broadcasted_iota(jnp.int32, (total, total), 0)
    new_hot = (at == new_ref[...]).astype(jnp.bfloat16)
    old_hot = (at == old_ref[...]).astype(jnp.bfloat16)
    moves = jnp.dot(new_hot, old_hot, preferred_element_type=jnp.float32).astype(jnp.bfloat16)
    wide[...] = recv_ref[...].astype(jnp.float32).reshape(wide.shape)
    for j in range(8):
        rows = wide[pl.ds(j, total, stride=8), :].astype(jnp.bfloat16)
        moved = lax.dot_general(
            rows, moves, (((0,), (1,)), ((), ())), preferred_element_type=jnp.float32
        ).astype(jnp.bfloat16)
        out_ref[j] = moved[:64]
        out_ref[j + 8] = moved[64:]


def solution(mesh):
    rows, cols = mesh.shape["row"], mesh.shape["col"]
    total = rows * cols

    def local(tables, bags, old_map, new_map):
        _, entries, width = tables.shape
        _, pool, batch = bags.shape
        per_row = batch // rows
        chunks = 8
        block = (total, 8, 128)
        recv = pl.pallas_call(
            functools.partial(pool_and_send, (rows, cols, per_row, pool, chunks)),
            out_shape=jax.ShapeDtypeStruct(block, jnp.bfloat16),
            in_specs=[pl.BlockSpec(memory_space=pl.ANY)] * 2,
            out_specs=pl.BlockSpec(memory_space=pltpu.VMEM),
            scratch_shapes=[
                pltpu.SMEM((pool, batch), jnp.int32),
                pltpu.VMEM((entries, width), jnp.bfloat16),
                pltpu.VMEM((entries, 128), jnp.float32),
                pltpu.VMEM((16, 128), jnp.float32),
                pltpu.VMEM(block, jnp.bfloat16),
                pltpu.SemaphoreType.DMA,
                pltpu.SemaphoreType.DMA((chunks,)),
                pltpu.SemaphoreType.DMA,
                pltpu.SemaphoreType.DMA,
            ],
            compiler_params=pltpu.CompilerParams(collective_id=0, has_side_effects=True),
        )(bags, tables)
        out = pl.pallas_call(
            place,
            out_shape=jax.ShapeDtypeStruct((per_row, width // cols, total), jnp.bfloat16),
            in_specs=[pl.BlockSpec(memory_space=pltpu.VMEM)] * 3,
            out_specs=pl.BlockSpec(memory_space=pltpu.VMEM),
            scratch_shapes=[pltpu.VMEM((total * 8, 128), jnp.float32)],
        )(old_map.reshape(1, total), new_map.reshape(1, total), recv)
        return jnp.swapaxes(out, 1, 2)

    return jax.shard_map(
        local,
        mesh=mesh,
        in_specs=(P(("row", "col"), None, None), P("row", None, None), P(), P()),
        out_specs=P("row", None, "col"),
        check_vma=False,
    )
```

```python
import functools

import jax
import jax.numpy as jnp
from jax import lax
from jax.experimental import pallas as pl
from jax.experimental.pallas import tpu as pltpu
from jax.sharding import PartitionSpec as P

MESH = pl.DeviceIdType.MESH
HIGH = 4096.0


def pool_and_send(dims, bags_ref, table_ref, recv_ref, bags, raw, packed, pooled, send, bag_sem, table_sem, send_sem, recv_sem):
    rows, cols, per_row, pool, chunks = dims
    row, col = lax.axis_index("row"), lax.axis_index("col")
    me = row * cols + col
    total = rows * cols
    chunk = raw.shape[0] // chunks

    def table_copy(c):
        part = pl.ds(c * chunk, chunk)
        return pltpu.make_async_copy(table_ref.at[0, part, :], raw.at[part, :], table_sem.at[c])

    count = bags.shape[0]
    bag_copy = pltpu.make_async_copy(bags_ref.at[pl.ds(col * count, count)], bags, bag_sem)
    bag_copy.start()
    for c in range(chunks):
        table_copy(c).start()

    barrier = pltpu.get_barrier_semaphore()

    def signal(r, k):
        pl.semaphore_signal(barrier, inc=1, device_id=(r, k), device_id_type=MESH)

    def greet(i, _):
        for k in range(cols):
            signal((row + i) & (rows - 1), k)
        return 0

    lax.fori_loop(1, rows, greet, 0)
    for d in range(1, cols):
        signal(row, (col + d) & (cols - 1))

    for c in range(chunks):
        table_copy(c).wait()

        def pack(i, _):
            at = pl.ds(pl.multiple_of(c * chunk + i * 256, 256), 256)
            pair = raw[at, :].astype(jnp.float32)
            packed[at, :] = pair[:, :128] + pair[:, 128:] * HIGH
            return 0

        lax.fori_loop(0, chunk // 256, pack, 0)
    bag_copy.wait()

    def destination(i):
        return (row + 1 + i) & (rows - 1)

    def copy_to(r, k):
        return pltpu.make_async_remote_copy(
            src_ref=send.at[r * cols + k],
            dst_ref=recv_ref.at[me],
            send_sem=send_sem,
            recv_sem=recv_sem,
            device_id=(r, k),
            device_id_type=MESH,
        )

    def send_pair(i):
        for half in range(2):
            for k in range(4):
                copy_to(destination(2 * i + half), k).start()

    def gather(i):
        for half in range(2):
            r = destination(2 * i + half)
            base = (r >> 3) * (pool * 128) + (r & 7) * per_row
            listed = [bags.at[pl.ds(base + l * 128, per_row)] for l in range(pool)]
            for j in range(per_row):
                parts = [packed[pl.ds(listed[l][j], 1), :] for l in range(pool)]
                while len(parts) > 1:
                    parts = [parts[n] + parts[n + 1] for n in range(0, len(parts), 2)]
                pooled[pl.ds(half * per_row + j, 1), :] = parts[0]
        return tuple(pooled[pl.ds(8 * n, 8), :] for n in range(4))

    def quantize(i, sums):
        first = lax.broadcasted_iota(jnp.int32, (8, 128), 1) < 64
        for half in range(2):
            parts = []
            for s in sums[2 * half : 2 * half + 2]:
                high = jnp.floor(s * (64.0 / HIGH) + 0.5)
                parts.append((s - high * (HIGH / 64.0), high * (1.0 / 64.0)))
            target = destination(2 * i + half) * cols
            for k in range(4):
                top, bottom = parts[0][k // 2], parts[1][k // 2]
                if k % 2 == 0:
                    block = jnp.where(first, top, pltpu.roll(bottom, 64, 1))
                else:
                    block = jnp.where(first, pltpu.roll(top, 64, 1), bottom)
                size = jnp.abs(block)
                left = jnp.max(jnp.where(first, size, 0.0), axis=1, keepdims=True)
                right = jnp.max(jnp.where(first, 0.0, size), axis=1, keepdims=True)
                scale = jnp.where(first, left, right) + 0.0078125
                levels = jnp.floor(block * (127.0 / scale) + 0.5)
                send[target + k] = (levels * scale / 127.0).astype(jnp.bfloat16)

    steps = rows // 2
    sums = gather(0)
    quantize(0, sums)
    sums = gather(1)
    pl.semaphore_wait(barrier, total - 1)

    def body(i, sums):
        send_pair(i - 2)
        quantize(i - 1, sums)
        return gather(i)

    sums = lax.fori_loop(2, steps, body, sums)
    send_pair(steps - 2)
    quantize(steps - 1, sums)
    recv_ref[me] = send[me]
    for k in range(4):
        copy_to(destination(rows - 2), k).start()
    for k in range(4):

        @pl.when(col != k)
        def _():
            copy_to(row, k).start()

    others = pl.ds(0, total - 1)
    done = pltpu.make_async_remote_copy(
        src_ref=send.at[others],
        dst_ref=recv_ref.at[others],
        send_sem=send_sem,
        recv_sem=recv_sem,
        device_id=(row, lax.rem(col + 1, cols)),
        device_id_type=MESH,
    )
    done.wait()


def place(old_ref, new_ref, recv_ref, out_ref, wide):
    total = recv_ref.shape[0]
    at = lax.broadcasted_iota(jnp.int32, (total, total), 0)
    new_hot = (at == new_ref[...]).astype(jnp.bfloat16)
    old_hot = (at == old_ref[...]).astype(jnp.bfloat16)
    moves = jnp.dot(new_hot, old_hot, preferred_element_type=jnp.float32).astype(jnp.bfloat16)
    wide[...] = recv_ref[...].astype(jnp.float32).reshape(wide.shape)
    for j in range(8):
        rows = wide[pl.ds(j, total, stride=8), :].astype(jnp.bfloat16)
        moved = lax.dot_general(
            rows, moves, (((0,), (1,)), ((), ())), preferred_element_type=jnp.float32
        ).astype(jnp.bfloat16)
        out_ref[j] = moved[:64]
        out_ref[j + 8] = moved[64:]


def solution(mesh):
    rows, cols = mesh.shape["row"], mesh.shape["col"]
    total = rows * cols

    def local(tables, bags, old_map, new_map):
        _, entries, width = tables.shape
        _, pool, batch = bags.shape
        per_row = batch // rows
        chunks = 8
        block = (total, 8, 128)
        listed = bags.reshape(cols, pool, batch // 128, 128).swapaxes(1, 2).reshape(-1)
        recv = pl.pallas_call(
            functools.partial(pool_and_send, (rows, cols, per_row, pool, chunks)),
            out_shape=jax.ShapeDtypeStruct(block, jnp.bfloat16),
            in_specs=[pl.BlockSpec(memory_space=pltpu.HBM)] * 2,
            out_specs=pl.BlockSpec(memory_space=pltpu.VMEM),
            scratch_shapes=[
                pltpu.SMEM((pool * batch,), jnp.int32),
                pltpu.VMEM((entries, width), jnp.bfloat16),
                pltpu.VMEM((entries, 128), jnp.float32),
                pltpu.VMEM((32, 128), jnp.float32),
                pltpu.VMEM(block, jnp.bfloat16),
                pltpu.SemaphoreType.DMA,
                pltpu.SemaphoreType.DMA((chunks,)),
                pltpu.SemaphoreType.DMA,
                pltpu.SemaphoreType.DMA,
            ],
            compiler_params=pltpu.CompilerParams(collective_id=0, has_side_effects=True, vmem_limit_bytes=16 << 20),
        )(pltpu.with_memory_space_constraint(listed, pltpu.HBM), pltpu.with_memory_space_constraint(tables, pltpu.HBM))
        out = pl.pallas_call(
            place,
            out_shape=jax.ShapeDtypeStruct((per_row, width // cols, total), jnp.bfloat16),
            in_specs=[pl.BlockSpec(memory_space=pltpu.VMEM)] * 3,
            out_specs=pl.BlockSpec(memory_space=pltpu.VMEM),
            scratch_shapes=[pltpu.VMEM((total * 8, 128), jnp.float32)],
            compiler_params=pltpu.CompilerParams(vmem_limit_bytes=16 << 20),
        )(old_map.reshape(1, total), new_map.reshape(1, total), recv)
        return jnp.swapaxes(out, 1, 2)

    return jax.shard_map(
        local,
        mesh=mesh,
        in_specs=(P(("row", "col"), None, None), P("row", None, None), P(), P()),
        out_specs=P("row", None, "col"),
        check_vma=False,
    )
```

```python
import functools

import jax
import jax.numpy as jnp
from jax import lax
from jax.experimental import pallas as pl
from jax.experimental.pallas import tpu as pltpu
from jax.sharding import PartitionSpec as P

MESH = pl.DeviceIdType.MESH
HIGH = 4096.0


def pool_and_send(dims, bags_ref, table_ref, recv_ref, bags, raw, packed, pooled, send, bag_sem, table_sem, send_sem, recv_sem, class_sem):
    rows, cols, per_row, pool, chunks = dims
    row, col = lax.axis_index("row"), lax.axis_index("col")
    me = row * cols + col
    total = rows * cols
    chunk = raw.shape[0] // chunks

    def table_copy(c):
        part = pl.ds(c * chunk, chunk)
        return pltpu.make_async_copy(table_ref.at[0, part, :], raw.at[part, :], table_sem.at[c])

    count = bags.shape[0]
    bag_copy = pltpu.make_async_copy(bags_ref.at[pl.ds(col * count, count)], bags, bag_sem)
    bag_copy.start()
    for c in range(chunks):
        table_copy(c).start()

    barrier = pltpu.get_barrier_semaphore()

    def signal(r, k):
        pl.semaphore_signal(barrier, inc=1, device_id=(r, k), device_id_type=MESH)

    z, y = row & 7, (row >> 3) & 3
    own_class = jnp.where(z < 4, z >> 1, 2 + (y >> 1))

    def greet(i, _):
        signal((row + i) & (rows - 1), own_class)
        return 0

    lax.fori_loop(1, rows, greet, 0, unroll=3)
    for d in range(1, cols):
        signal(row, (col + d) & (cols - 1))

    def class_is_in(c):
        @pl.when(col == c)
        def _():
            pl.semaphore_wait(barrier, jnp.where(own_class == c, total // 4 - 1, total // 4 + cols - 1))
            for d in range(1, cols):
                pl.semaphore_signal(
                    class_sem.at[c], inc=1, device_id=(row, (c + d) % cols), device_id_type=MESH
                )

        @pl.when(col != c)
        def _():
            pl.semaphore_wait(class_sem.at[c], 1)

    for c in range(chunks):
        table_copy(c).wait()

        def pack(i, _):
            at = pl.ds(pl.multiple_of(c * chunk + i * 256, 256), 256)
            pair = raw[at, :].astype(jnp.float32)
            packed[at, :] = pair[:, :128] + pair[:, 128:] * HIGH
            return 0

        lax.fori_loop(0, chunk // 256, pack, 0)
    bag_copy.wait()

    def destination(i):
        c, u = i >> 4, i & 15
        near = (u >> 1) * 8 + c * 2 + ((u + z) & 1)
        far = (u >> 3) * 32 + (c & 1) * 16 + ((u >> 2) & 1) * 8 + 4 + ((u + z) & 3)
        return jnp.where(i < rows // 2, near, far)

    def pair(p):
        return destination(2 * p), destination(2 * p + 1)

    def send_to(r, k):
        own = (r == row) & (col == k)
        pltpu.make_async_remote_copy(
            src_ref=send.at[r * cols + k],
            dst_ref=recv_ref.at[jnp.where(own, total, me)],
            send_sem=send_sem,
            recv_sem=recv_sem,
            device_id=(r, jnp.where(own, k ^ 1, k)),
            device_id_type=MESH,
        ).start()

    def send_pair(targets):
        for r in targets:
            for k in range(cols):
                send_to(r, k)

    def gather(targets):
        for half, r in enumerate(targets):
            base = (r >> 3) * (pool * 128) + (r & 7) * per_row
            listed = [bags.at[pl.ds(base + l * 128, per_row)] for l in range(pool)]
            for j in range(per_row):
                parts = [packed[pl.ds(listed[l][j], 1), :] for l in range(pool)]
                while len(parts) > 1:
                    parts = [parts[n] + parts[n + 1] for n in range(0, len(parts), 2)]
                pooled[pl.ds(half * per_row + j, 1), :] = parts[0]
        return tuple(pooled[pl.ds(8 * n, 8), :] for n in range(4))

    def quantize(targets, sums):
        first = lax.broadcasted_iota(jnp.int32, (8, 128), 1) < 64
        for half in range(2):
            parts = []
            for s in sums[2 * half : 2 * half + 2]:
                high = jnp.floor(s * (64.0 / HIGH) + 0.5)
                parts.append((s - high * (HIGH / 64.0), high * (1.0 / 64.0)))
            target = targets[half] * cols
            for k in range(4):
                top, bottom = parts[0][k // 2], parts[1][k // 2]
                if k % 2 == 0:
                    block = jnp.where(first, top, pltpu.roll(bottom, 64, 1))
                else:
                    block = jnp.where(first, pltpu.roll(top, 64, 1), bottom)
                size = jnp.abs(block)
                left = jnp.max(jnp.where(first, size, 0.0), axis=1, keepdims=True)
                right = jnp.max(jnp.where(first, 0.0, size), axis=1, keepdims=True)
                scale = jnp.where(first, left, right) + 0.0078125
                levels = jnp.floor(block * (127.0 / scale) + 0.5)
                send[target + k] = (levels * scale / 127.0).astype(jnp.bfloat16)

    steps = rows // 2
    older, old = pair(0), pair(1)
    sums = gather(older)
    quantize(older, sums)
    sums = gather(old)

    def body(p, carry):
        older, old, sums = carry
        new = pair(p)
        send_pair(older)
        quantize(old, sums)
        return old, new, gather(new)

    carry = older, old, sums
    for c in range(4):
        class_is_in(c)
        start = 2 + c * (steps // 4)
        carry = lax.fori_loop(start, min(start + steps // 4, steps), body, carry)
    older, old, sums = carry
    send_pair(older)
    quantize(old, sums)
    recv_ref[me] = send[me]
    send_pair(old)

    others = pl.ds(0, total)
    done = pltpu.make_async_remote_copy(
        src_ref=send.at[others],
        dst_ref=recv_ref.at[others],
        send_sem=send_sem,
        recv_sem=recv_sem,
        device_id=(row, lax.rem(col + 1, cols)),
        device_id_type=MESH,
    )
    done.wait()


def place(old_ref, new_ref, recv_ref, out_ref, wide):
    total = old_ref.shape[1]
    at = lax.broadcasted_iota(jnp.int32, (total, total), 0)
    new_hot = (at == new_ref[...]).astype(jnp.bfloat16)
    old_hot = (at == old_ref[...]).astype(jnp.bfloat16)
    moves = jnp.dot(new_hot, old_hot, preferred_element_type=jnp.float32).astype(jnp.bfloat16)
    wide[...] = recv_ref[:total].astype(jnp.float32).reshape(wide.shape)
    for j in range(8):
        rows = wide[pl.ds(j, total, stride=8), :].astype(jnp.bfloat16)
        moved = lax.dot_general(
            rows, moves, (((0,), (1,)), ((), ())), preferred_element_type=jnp.float32
        ).astype(jnp.bfloat16)
        out_ref[j] = moved[:64]
        out_ref[j + 8] = moved[64:]


def solution(mesh):
    rows, cols = mesh.shape["row"], mesh.shape["col"]
    total = rows * cols

    def local(tables, bags, old_map, new_map):
        _, entries, width = tables.shape
        _, pool, batch = bags.shape
        per_row = batch // rows
        chunks = 8
        block = (total, 8, 128)
        listed = bags.reshape(cols, pool, batch // 128, 128).swapaxes(1, 2).reshape(-1)
        recv = pl.pallas_call(
            functools.partial(pool_and_send, (rows, cols, per_row, pool, chunks)),
            out_shape=jax.ShapeDtypeStruct((total + 1, 8, 128), jnp.bfloat16),
            in_specs=[pl.BlockSpec(memory_space=pltpu.HBM)] * 2,
            out_specs=pl.BlockSpec(memory_space=pltpu.VMEM),
            scratch_shapes=[
                pltpu.SMEM((pool * batch,), jnp.int32),
                pltpu.VMEM((entries, width), jnp.bfloat16),
                pltpu.VMEM((entries, 128), jnp.float32),
                pltpu.VMEM((32, 128), jnp.float32),
                pltpu.VMEM(block, jnp.bfloat16),
                pltpu.SemaphoreType.DMA,
                pltpu.SemaphoreType.DMA((chunks,)),
                pltpu.SemaphoreType.DMA,
                pltpu.SemaphoreType.DMA,
                pltpu.SemaphoreType.REGULAR((4,)),
            ],
            compiler_params=pltpu.CompilerParams(collective_id=0, has_side_effects=True, vmem_limit_bytes=16 << 20),
        )(pltpu.with_memory_space_constraint(listed, pltpu.HBM), pltpu.with_memory_space_constraint(tables, pltpu.HBM))
        out = pl.pallas_call(
            place,
            out_shape=jax.ShapeDtypeStruct((per_row, width // cols, total), jnp.bfloat16),
            in_specs=[pl.BlockSpec(memory_space=pltpu.VMEM)] * 3,
            out_specs=pl.BlockSpec(memory_space=pltpu.VMEM),
            scratch_shapes=[pltpu.VMEM((total * 8, 128), jnp.float32)],
            compiler_params=pltpu.CompilerParams(vmem_limit_bytes=16 << 20),
        )(old_map.reshape(1, total), new_map.reshape(1, total), recv)
        return jnp.swapaxes(out, 1, 2)

    return jax.shard_map(
        local,
        mesh=mesh,
        in_specs=(P(("row", "col"), None, None), P("row", None, None), P(), P()),
        out_specs=P("row", None, "col"),
        check_vma=False,
    )
```

```python
import functools

import jax
import jax.numpy as jnp
from jax import lax
from jax.experimental import pallas as pl
from jax.experimental.pallas import tpu as pltpu
from jax.sharding import PartitionSpec as P

MESH = pl.DeviceIdType.MESH
HIGH = 4096.0


def pool_and_send(dims, bags_ref, table_ref, recv_ref, bags, raw, packed, pooled, send, bag_sem, table_sem, send_sem, recv_sem, class_sem):
    rows, cols, per_row, pool, chunks = dims
    row, col = lax.axis_index("row"), lax.axis_index("col")
    me = row * cols + col
    total = rows * cols
    chunk = raw.shape[0] // chunks

    def table_copy(c):
        part = pl.ds(c * chunk, chunk)
        return pltpu.make_async_copy(table_ref.at[0, part, :], raw.at[part, :], table_sem.at[c])

    count = bags.shape[0]
    bag_copy = pltpu.make_async_copy(bags_ref.at[pl.ds(col * count, count)], bags, bag_sem)
    bag_copy.start()
    for c in range(chunks):
        table_copy(c).start()

    barrier = pltpu.get_barrier_semaphore()

    def signal(r, k):
        pl.semaphore_signal(barrier, inc=1, device_id=(r, k), device_id_type=MESH)

    z, y = row & 7, (row >> 3) & 3
    own_class = jnp.where(z < 4, z >> 1, 2 + (y >> 1))
    members = (rows // 4,) * 4

    def greet(i, _):
        signal((row + i) & (rows - 1), own_class ^ 2)
        return 0

    lax.fori_loop(1, rows, greet, 0, unroll=3)
    for d in range(1, cols):
        signal(row, (col + d) & (cols - 1))

    def class_is_in(c):
        @pl.when(col == c ^ 2)
        def _():
            pl.semaphore_wait(barrier, members[c] * cols + jnp.where(own_class == c, -1, cols - 1))
            for d in range(1, cols):
                pl.semaphore_signal(
                    class_sem.at[c], inc=1, device_id=(row, ((c ^ 2) + d) % cols), device_id_type=MESH
                )

        @pl.when(col != c ^ 2)
        def _():
            pl.semaphore_wait(class_sem.at[c], 1)

    for c in range(chunks):
        table_copy(c).wait()

        def pack(i, _):
            at = pl.ds(pl.multiple_of(c * chunk + i * 256, 256), 256)
            pair = raw[at, :].astype(jnp.float32)
            packed[at, :] = pair[:, :128] + pair[:, 128:] * HIGH
            return 0

        lax.fori_loop(0, chunk // 256, pack, 0)
    bag_copy.wait()

    def destination(i):
        near = ((i >> 1) & 7) * 8 + ((i >> 4) << 1) + ((i + z) & 1)
        far = ((i >> 3) & 1) * 32 + ((i >> 4) & 1) * 16 + ((i >> 2) & 1) * 8 + 4 + ((i + z) & 3)
        return jnp.where(i < rows // 2, near, far)

    def pair(p):
        return destination(2 * p), destination(2 * p + 1)

    def send_to(r, k):
        own = (r == row) & (col == k)
        pltpu.make_async_remote_copy(
            src_ref=send.at[r * cols + k],
            dst_ref=recv_ref.at[jnp.where(own, total, me)],
            send_sem=send_sem,
            recv_sem=recv_sem,
            device_id=(r, jnp.where(own, k ^ 1, k)),
            device_id_type=MESH,
        ).start()

    def send_pair(targets):
        for r in targets:
            for k in range(cols):
                send_to(r, k)

    def gather(targets):
        for half, r in enumerate(targets):
            base = (r >> 3) * (pool * 128) + (r & 7) * per_row
            listed = [bags.at[pl.ds(base + l * 128, per_row)] for l in range(pool)]
            for j in range(per_row):
                parts = [packed[pl.ds(listed[l][j], 1), :] for l in range(pool)]
                while len(parts) > 1:
                    parts = [parts[n] + parts[n + 1] for n in range(0, len(parts), 2)]
                pooled[pl.ds(half * per_row + j, 1), :] = parts[0]
        return tuple(pooled[pl.ds(n, 8, stride=2), :] for n in (0, 1, 16, 17))

    def quantize(targets, sums):
        first = lax.broadcasted_iota(jnp.int32, (8, 128), 1) < 64
        for half in range(2):
            parts = []
            for s in sums[2 * half : 2 * half + 2]:
                high = jnp.floor(s * (64.0 / HIGH) + 0.5)
                parts.append((s - high * (HIGH / 64.0), high * (1.0 / 64.0)))
            target = targets[half] * cols
            for k in range(4):
                top, bottom = parts[0][k // 2], parts[1][k // 2]
                if k % 2 == 0:
                    block = jnp.where(first, top, pltpu.roll(bottom, 64, 1))
                else:
                    block = jnp.where(first, pltpu.roll(top, 64, 1), bottom)
                size = jnp.abs(block)
                left = jnp.max(jnp.where(first, size, 0.0), axis=1, keepdims=True)
                right = jnp.max(jnp.where(first, 0.0, size), axis=1, keepdims=True)
                scale = jnp.where(first, left, right) + 0.0078125
                levels = jnp.floor(block * (127.0 / scale) + 0.5)
                send[target + k] = (levels * scale / 127.0).astype(jnp.bfloat16)

    steps = rows // 2
    older, old = pair(0), pair(1)
    sums = gather(older)
    quantize(older, sums)
    sums = gather(old)

    def body(p, carry):
        older, old, sums = carry
        new = pair(p)
        send_pair(older)
        quantize(old, sums)
        return old, new, gather(new)

    carry, start = (older, old, sums), 2
    for c in range(4):
        class_is_in(c)
        stop = min(start + members[c] // 2, steps)
        carry = lax.fori_loop(start, stop, body, carry)
        start = stop
    older, old, sums = carry
    send_pair(older)
    quantize(old, sums)
    recv_ref[me] = send[me]
    send_pair(old)

    others = pl.ds(0, total)
    done = pltpu.make_async_remote_copy(
        src_ref=send.at[others],
        dst_ref=recv_ref.at[others],
        send_sem=send_sem,
        recv_sem=recv_sem,
        device_id=(row, lax.rem(col + 1, cols)),
        device_id_type=MESH,
    )
    done.wait()


def place(old_ref, new_ref, recv_ref, out_ref, wide, placed, sems):
    total = old_ref.shape[1]
    at = lax.broadcasted_iota(jnp.int32, (total, total), 0)
    new_hot = (at == new_ref[...]).astype(jnp.bfloat16)
    old_hot = (at == old_ref[...]).astype(jnp.bfloat16)
    moves = jnp.dot(new_hot, old_hot, preferred_element_type=jnp.float32).astype(jnp.bfloat16)
    wide[...] = recv_ref[:total].astype(jnp.float32).reshape(wide.shape)
    copies = []
    for j in range(8):
        rows = wide[pl.ds(j, total, stride=8), :].astype(jnp.bfloat16)
        moved = lax.dot_general(
            rows, moves, (((0,), (1,)), ((), ())), preferred_element_type=jnp.float32
        ).astype(jnp.bfloat16)
        placed[2 * j] = moved[:64]
        placed[2 * j + 1] = moved[64:]
        if j % 2 == 1:
            part = pl.ds(2 * j - 2, 4)
            copies.append(pltpu.make_async_copy(placed.at[part], out_ref.at[part], sems.at[j // 2]))
            copies[-1].start()
    for copy in copies:
        copy.wait()


def solution(mesh):
    rows, cols = mesh.shape["row"], mesh.shape["col"]
    total = rows * cols

    def local(tables, bags, old_map, new_map):
        _, entries, width = tables.shape
        _, pool, batch = bags.shape
        per_row = batch // rows
        chunks = 8
        block = (total, 8, 128)
        listed = bags.reshape(cols, pool, batch // 128, 128).swapaxes(1, 2).reshape(-1)
        recv = pl.pallas_call(
            functools.partial(pool_and_send, (rows, cols, per_row, pool, chunks)),
            out_shape=jax.ShapeDtypeStruct((total + 1, 8, 128), jnp.bfloat16),
            in_specs=[pl.BlockSpec(memory_space=pltpu.HBM)] * 2,
            out_specs=pl.BlockSpec(memory_space=pltpu.VMEM),
            scratch_shapes=[
                pltpu.SMEM((pool * batch,), jnp.int32),
                pltpu.VMEM((entries, width), jnp.bfloat16),
                pltpu.VMEM((entries, 128), jnp.float32),
                pltpu.VMEM((32, 128), jnp.float32),
                pltpu.VMEM(block, jnp.bfloat16),
                pltpu.SemaphoreType.DMA,
                pltpu.SemaphoreType.DMA((chunks,)),
                pltpu.SemaphoreType.DMA,
                pltpu.SemaphoreType.DMA,
                pltpu.SemaphoreType.REGULAR((4,)),
            ],
            compiler_params=pltpu.CompilerParams(collective_id=0, has_side_effects=True, vmem_limit_bytes=16 << 20),
        )(pltpu.with_memory_space_constraint(listed, pltpu.HBM), pltpu.with_memory_space_constraint(tables, pltpu.HBM))
        out = pl.pallas_call(
            place,
            out_shape=jax.ShapeDtypeStruct((per_row, width // cols, total), jnp.bfloat16),
            in_specs=[pl.BlockSpec(memory_space=pltpu.VMEM)] * 3,
            out_specs=pl.BlockSpec(memory_space=pl.ANY),
            scratch_shapes=[
                pltpu.VMEM((total * 8, 128), jnp.float32),
                pltpu.VMEM((per_row, width // cols, total), jnp.bfloat16),
                pltpu.SemaphoreType.DMA((4,)),
            ],
            compiler_params=pltpu.CompilerParams(vmem_limit_bytes=16 << 20),
        )(old_map.reshape(1, total), new_map.reshape(1, total), recv)
        return jnp.swapaxes(out, 1, 2)

    return jax.shard_map(
        local,
        mesh=mesh,
        in_specs=(P(("row", "col"), None, None), P("row", None, None), P(), P()),
        out_specs=P("row", None, "col"),
        check_vma=False,
    )
```

```python
import functools

import jax
import jax.numpy as jnp
from jax import lax
from jax.experimental import pallas as pl
from jax.experimental.pallas import tpu as pltpu
from jax.sharding import PartitionSpec as P

MESH = pl.DeviceIdType.MESH
HIGH = 4096.0


def pool_and_send(dims, bags_ref, table_ref, recv_ref, bags, raw, packed, pooled, send, bag_sem, table_sem, send_sem, recv_sem, class_sem):
    rows, cols, per_row, pool, chunks = dims
    row, col = lax.axis_index("row"), lax.axis_index("col")
    me = row * cols + col
    total = rows * cols
    chunk = raw.shape[0] // chunks

    def table_copy(c):
        part = pl.ds(c * chunk, chunk)
        return pltpu.make_async_copy(table_ref.at[0, part, :], raw.at[part, :], table_sem.at[c])

    count = bags.shape[0]
    bag_copy = pltpu.make_async_copy(bags_ref.at[pl.ds(col * count, count)], bags, bag_sem)
    bag_copy.start()
    for c in range(chunks):
        table_copy(c).start()

    barrier = pltpu.get_barrier_semaphore()

    def signal(r, k):
        pl.semaphore_signal(barrier, inc=1, device_id=(r, k), device_id_type=MESH)

    z, y = row & 7, (row >> 3) & 3
    own_class = jnp.where(z < 4, z >> 1, 2 + (y >> 1))
    members = (rows // 4,) * 4

    def greet(i, _):
        signal((row + i) & (rows - 1), own_class ^ 2)
        return 0

    lax.fori_loop(1, rows, greet, 0, unroll=3)
    for d in range(1, cols):
        signal(row, (col + d) & (cols - 1))

    def class_is_in(c):
        @pl.when(col == c ^ 2)
        def _():
            pl.semaphore_wait(barrier, members[c] * cols + jnp.where(own_class == c, -1, cols - 1))
            for d in range(1, cols):
                pl.semaphore_signal(
                    class_sem.at[c], inc=1, device_id=(row, ((c ^ 2) + d) % cols), device_id_type=MESH
                )

        @pl.when(col != c ^ 2)
        def _():
            pl.semaphore_wait(class_sem.at[c], 1)

    for c in range(chunks):
        table_copy(c).wait()

        def pack(i, _):
            at = pl.ds(pl.multiple_of(c * chunk + i * 256, 256), 256)
            pair = raw[at, :].astype(jnp.float32)
            packed[at, :] = pair[:, :128] + pair[:, 128:] * HIGH
            return 0

        lax.fori_loop(0, chunk // 256, pack, 0)
    bag_copy.wait()

    def destination(i):
        near = ((i >> 1) & 7) * 8 + ((i >> 4) << 1) + ((i + z) & 1)
        far = ((i >> 3) & 1) * 32 + ((i >> 4) & 1) * 16 + ((i >> 2) & 1) * 8 + 4 + ((i + z) & 3)
        return jnp.where(i < rows // 2, near, far)

    def pair(p):
        return destination(2 * p), destination(2 * p + 1)

    def send_to(r, k):
        own = (r == row) & (col == k)
        pltpu.make_async_remote_copy(
            src_ref=send.at[r * cols + k],
            dst_ref=recv_ref.at[jnp.where(own, total, me)],
            send_sem=send_sem,
            recv_sem=recv_sem,
            device_id=(r, jnp.where(own, k ^ 1, k)),
            device_id_type=MESH,
        ).start()

    def send_pair(targets):
        for r in targets:
            for k in range(cols):
                send_to(r, k)

    def gather(targets):
        for half, r in enumerate(targets):
            base = (r >> 3) * (pool * 128) + (r & 7) * per_row
            listed = [bags.at[pl.ds(base + l * 128, per_row)] for l in range(pool)]
            for j in range(per_row):
                parts = [packed[pl.ds(listed[l][j], 1), :] for l in range(pool)]
                while len(parts) > 1:
                    parts = [parts[n] + parts[n + 1] for n in range(0, len(parts), 2)]
                pooled[pl.ds(half * per_row + j, 1), :] = parts[0]
        return tuple(pooled[pl.ds(n, 8, stride=2), :] for n in (0, 1, 16, 17))

    def quantize(targets, sums):
        first = lax.broadcasted_iota(jnp.int32, (8, 128), 1) < 64
        for half in range(2):
            parts = []
            for s in sums[2 * half : 2 * half + 2]:
                high = jnp.floor(s * (64.0 / HIGH) + 0.5)
                parts.append((s - high * (HIGH / 64.0), high * (1.0 / 64.0)))
            target = targets[half] * cols
            for k in range(4):
                top, bottom = parts[0][k // 2], parts[1][k // 2]
                if k % 2 == 0:
                    block = jnp.where(first, top, pltpu.roll(bottom, 64, 1))
                else:
                    block = jnp.where(first, pltpu.roll(top, 64, 1), bottom)
                size = jnp.abs(block)
                left = jnp.max(jnp.where(first, size, 0.0), axis=1, keepdims=True)
                right = jnp.max(jnp.where(first, 0.0, size), axis=1, keepdims=True)
                scale = jnp.where(first, left, right) + 0.0078125
                levels = jnp.floor(block * (127.0 / scale) + 0.5)
                send[target + k] = (levels * scale / 127.0).astype(jnp.bfloat16)

    steps = rows // 2
    older, old = pair(0), pair(1)
    sums = gather(older)
    quantize(older, sums)
    sums = gather(old)

    def body(p, carry):
        older, old, sums = carry
        new = pair(p)
        send_pair(older)
        quantize(old, sums)
        return old, new, gather(new)

    carry, start = (older, old, sums), 2
    for c in range(4):
        class_is_in(c)
        stop = min(start + members[c] // 2, steps)
        carry = lax.fori_loop(start, stop, body, carry)
        start = stop
    older, old, sums = carry
    send_pair(older)
    quantize(old, sums)
    recv_ref[me] = send[me]
    send_pair(old)

    others = pl.ds(0, total)
    done = pltpu.make_async_remote_copy(
        src_ref=send.at[others],
        dst_ref=recv_ref.at[others],
        send_sem=send_sem,
        recv_sem=recv_sem,
        device_id=(row, lax.rem(col + 1, cols)),
        device_id_type=MESH,
    )
    done.wait()


def place(old_ref, new_ref, recv_ref, out_ref, wide, placed, sems):
    total = old_ref.shape[1]
    at = lax.broadcasted_iota(jnp.int32, (total, total), 0)
    new_hot = (at == new_ref[...]).astype(jnp.bfloat16)
    old_hot = (at == old_ref[...]).astype(jnp.bfloat16)
    moves = jnp.dot(new_hot, old_hot, preferred_element_type=jnp.float32).astype(jnp.bfloat16)
    wide[: 8 * total] = recv_ref[:total].astype(jnp.float32).reshape(8 * total, 128)
    copies = []
    for j in range(8):
        rows = wide[pl.ds(j, total, stride=8), :].astype(jnp.bfloat16)
        moved = lax.dot_general(
            rows, moves, (((0,), (1,)), ((), ())), preferred_element_type=jnp.float32
        ).astype(jnp.bfloat16)
        placed[2 * j] = moved[:64]
        placed[2 * j + 1] = moved[64:]
        part = pl.ds(2 * j, 2)
        copies.append(pltpu.make_async_copy(placed.at[part], out_ref.at[part], sems.at[j]))
        copies[-1].start()
    for copy in copies:
        copy.wait()


def solution(mesh):
    rows, cols = mesh.shape["row"], mesh.shape["col"]
    total = rows * cols

    def local(tables, bags, old_map, new_map):
        _, entries, width = tables.shape
        _, pool, batch = bags.shape
        per_row = batch // rows
        chunks = 8
        block = (total, 8, 128)
        listed = bags.reshape(cols, pool, batch // 128, 128).swapaxes(1, 2).reshape(-1)
        recv = pl.pallas_call(
            functools.partial(pool_and_send, (rows, cols, per_row, pool, chunks)),
            out_shape=jax.ShapeDtypeStruct((total + 1, 8, 128), jnp.bfloat16),
            in_specs=[pl.BlockSpec(memory_space=pltpu.HBM)] * 2,
            out_specs=pl.BlockSpec(memory_space=pltpu.VMEM),
            scratch_shapes=[
                pltpu.SMEM((pool * batch,), jnp.int32),
                pltpu.VMEM((entries, width), jnp.bfloat16),
                pltpu.VMEM((entries, 128), jnp.float32),
                pltpu.VMEM((40, 128), jnp.float32),
                pltpu.VMEM(block, jnp.bfloat16),
                pltpu.SemaphoreType.DMA,
                pltpu.SemaphoreType.DMA((chunks,)),
                pltpu.SemaphoreType.DMA,
                pltpu.SemaphoreType.DMA,
                pltpu.SemaphoreType.REGULAR((4,)),
            ],
            compiler_params=pltpu.CompilerParams(collective_id=0, has_side_effects=True, vmem_limit_bytes=16 << 20),
        )(pltpu.with_memory_space_constraint(listed, pltpu.HBM), pltpu.with_memory_space_constraint(tables, pltpu.HBM))
        out = pl.pallas_call(
            place,
            out_shape=jax.ShapeDtypeStruct((per_row, width // cols, total), jnp.bfloat16),
            in_specs=[pl.BlockSpec(memory_space=pltpu.VMEM)] * 3,
            out_specs=pl.BlockSpec(memory_space=pl.ANY),
            scratch_shapes=[
                pltpu.VMEM((total * 8 + 8, 128), jnp.float32),
                pltpu.VMEM((per_row, width // cols, total), jnp.bfloat16),
                pltpu.SemaphoreType.DMA((8,)),
            ],
            compiler_params=pltpu.CompilerParams(vmem_limit_bytes=16 << 20),
        )(old_map.reshape(1, total), new_map.reshape(1, total), recv)
        return jnp.swapaxes(out, 1, 2)

    return jax.shard_map(
        local,
        mesh=mesh,
        in_specs=(P(("row", "col"), None, None), P("row", None, None), P(), P()),
        out_specs=P("row", None, "col"),
        check_vma=False,
    )
```
